128 devices in a mesh: row: 8 (over x, core), col: 16 (over y, z).
Axes of the slice: x: 4, y: 4, z: 4, core: 2. Of those that a mesh axis runs over, the one named last changes fastest.
Arguments:
- matrix: float32 [6144, 6, 8192], P('row', None, 'col'), may hold values from -6 to 6
- factor: float32 [6, 8192, 2048], P(None, 'col', 'row'), as said below
Outputs:
- updated: float32 [6144, 6, 8192], P('row', None, 'col')
- solved: float32 [6144, 2048], P('row')
The draws below stay inside these ranges and needn't reach their ends.
Inputs may be any that keep to these rules, and one draw needn't show every extreme that they name: factor is lower trapezoidal: zero wherever the column index exceeds the row index; its diagonal entries lie in 1 to 2.
All inputs are finite; a program needn't handle non-finite values.
Results may differ from the reference program's by a relative error of at most 0.00013.
Values sent between devices are 32-bit elements; how exact they have to be, the bound alone decides.
No kernel may reach another device: no remote copies, remote signals or barrier semaphores. Data moves between devices by JAX's collectives and lax.ppermute only.
A program may use at most 256 MiB of HBM per device.

```python
import jax
import jax.numpy as jnp
from jax import lax

N = 49152
B = 512
P_SIZE = 4
M = 6144
LB = 6
N_COL = 16


def draw_factor(key, part):
    key_noise = jax.random.fold_in(key, 11)
    key_diag = jax.random.fold_in(key, 12)
    span = N // LB
    shape = (LB, span, P_SIZE * B)
    row_ids = jnp.arange(LB)[:, None, None] * span + jnp.arange(span)[None, :, None]
    col_ids = jnp.arange(P_SIZE * B)[None, None, :]
    noise = jax.random.normal(key_noise, shape, jnp.float32)
    same_block = row_ids // B == col_ids // B
    off_vals = jnp.where(same_block, 0.4, 1.0) * noise / jnp.sqrt(jnp.float32(B))
    diag_vals = jax.random.uniform(key_diag, shape, jnp.float32, 1.0, 2.0)
    lower_vals = jnp.where(row_ids > col_ids, off_vals, 0.0)
    return jnp.where(row_ids == col_ids, diag_vals, lower_vals).astype(jnp.float32)


def levels(own_key, shape, split, least, top_value):
    level = 1.0
    for axis_at, shards_of in split:
        heights = jax.random.uniform(jax.random.fold_in(jax.random.fold_in(own_key, 6), axis_at), (shards_of,), jnp.float32, least / len(split), top_value / len(split))
        level = level * jnp.repeat(jnp.exp(heights), shape[axis_at] // shards_of).reshape((-1,) + (1,) * (len(shape) - 1 - axis_at))
    return level


def bell_draw(stream_key, shape, spread, limit, shards=(), held_as=jnp.bfloat16):
    factor_of = levels(stream_key, shape, shards, -0.22, 0.18) if shards else 1.0
    values = jax.random.normal(stream_key, shape, jnp.float32) * spread * factor_of
    return jnp.minimum(jnp.maximum(values, -limit), limit).astype(held_as)


def setup_inputs(seed: int = 0) -> dict:
    seeds = jax.random.split(jax.random.key(seed), 3)
    return {
        "matrix": bell_draw(seeds[0], (M, LB, N_COL * B), 1.0, 6.0, ((0, 8), (2, 16)), jnp.float32),
        "factor": draw_factor(jax.random.fold_in(seeds[2], 71), 0),
    }


def reference(matrix, factor):
    row_count = matrix.shape[0]
    nblocks = N // B
    blocks = matrix.reshape(row_count, nblocks, B)
    factor_tiles = factor.reshape(nblocks, B, P_SIZE * B)
    panels = []
    for step in range(P_SIZE):
        right_side = blocks[:, step, :]
        if step > 0:
            earlier = jnp.concatenate(panels, axis=1)
            right_side = right_side - jnp.dot(earlier.astype(jnp.float32), factor_tiles[step, :, :step * B].T.astype(jnp.float32), precision=lax.Precision.HIGHEST, preferred_element_type=jnp.float32)
        diag_tile = factor_tiles[step, :, step * B:(step + 1) * B]
        solved_block = lax.linalg.triangular_solve(diag_tile, right_side, left_side=False, lower=True, transpose_a=True)
        panels.append(solved_block)
    solved = jnp.concatenate(panels, axis=1)
    block_of_row = (jnp.arange(N) // B).astype(jnp.int32)
    panel_of_col = (jnp.arange(P_SIZE * B) // B).astype(jnp.int32)
    active = panel_of_col[None, :] < block_of_row[:, None]
    masked = jnp.where(active, factor.reshape(N, P_SIZE * B), jnp.zeros((), factor.dtype))
    updated = matrix.reshape(row_count, N) - jnp.dot(solved.astype(jnp.float32), masked.T.astype(jnp.float32), precision=lax.Precision.HIGHEST, preferred_element_type=jnp.float32)
    return (updated.reshape(matrix.shape), solved)
```

```python
import functools

import jax
import jax.numpy as jnp
from jax import lax
from jax.experimental import pallas as pl
from jax.experimental.pallas import tpu as pltpu
from jax.sharding import Mesh
from jax.sharding import PartitionSpec as P


ROW = ("x", "core")
COL = ("y", "z")
SWAP = [(0, 1), (1, 0)]
HIGHEST = lax.Precision.HIGHEST


def full_dot(a, b):
    return jnp.dot(a, b, precision=HIGHEST, preferred_element_type=jnp.float32)


def dot_nt(a, b):
    return lax.dot_general(
        a, b, (((1,), (1,)), ((), ())), precision=HIGHEST, preferred_element_type=jnp.float32
    )


def inverse_into(tile_ref, out_ref):
    size, wide, small = 512, 128, 16
    parts = size // wide
    diag = jnp.concatenate(
        [tile_ref[wide * p : wide * (p + 1), wide * p : wide * (p + 1)] for p in range(parts)], axis=0
    )
    row = lax.broadcasted_iota(jnp.int32, (size, wide), 0)
    lane = lax.broadcasted_iota(jnp.int32, (size, wide), 1)
    local_row = row % wide
    lower = jnp.where(lane <= local_row, diag, 0.0)
    own = jnp.sum(jnp.where(lane == local_row, lower, 0.0), axis=1, keepdims=True)
    unit = lower / own
    inverse = jnp.where(lane == local_row, 1.0, 0.0)
    block_start = (local_row // small) * small
    inverse = inverse.reshape(size // small, small, wide)
    for i in range(small - 1):
        picked = jnp.where((lane == block_start + i) & (local_row > lane), unit, 0.0)
        weight = jnp.sum(picked, axis=1, keepdims=True).reshape(size // small, small, 1)
        inverse = inverse - weight * inverse[:, i : i + 1, :]
    inverse = inverse.reshape(size, wide)
    r1 = lax.broadcasted_iota(jnp.int32, (wide, wide), 0)
    c1 = lax.broadcasted_iota(jnp.int32, (wide, wide), 1)
    invs = [inverse[wide * p : wide * (p + 1)] for p in range(parts)]
    step = small
    while step < wide:
        keep = (r1 // (2 * step) == c1 // (2 * step)) & (r1 // step > c1 // step)
        offs = [jnp.where(keep, unit[wide * p : wide * (p + 1)], 0.0) for p in range(parts)]
        mids = [full_dot(offs[p], invs[p]) for p in range(parts)]
        invs = [invs[p] - full_dot(invs[p], mids[p]) for p in range(parts)]
        step *= 2
    out_ref[...] = jnp.zeros((size, size), jnp.float32)
    for p in range(parts):
        scale = jnp.broadcast_to(1.0 / own[wide * p : wide * (p + 1)], (wide, wide))
        as_row = jnp.sum(jnp.where(r1 == c1, scale, 0.0), axis=0, keepdims=True)
        out_ref[wide * p : wide * (p + 1), wide * p : wide * (p + 1)] = invs[p] * as_row
    step = wide
    while step < size:
        for s in range(0, size, 2 * step):
            top = out_ref[s : s + step, s : s + step]
            bottom = out_ref[s + step : s + 2 * step, s + step : s + 2 * step]
            between = tile_ref[s + step : s + 2 * step, s : s + step]
            out_ref[s + step : s + 2 * step, s : s + step] = -full_dot(bottom, full_dot(between, top))
        step *= 2


def prepare_body(place_ref, rows_ref, *refs):
    near, far = refs[:4], refs[4:8]
    panel_ref, inverse_ref, first_ref = refs[8:]
    core, y, z = place_ref[0], place_ref[1], place_ref[2]
    for c in range(2):

        @pl.when(core == c)
        def _():
            for d in range(4):
                at = pl.multiple_of(lax.rem(y + (4 - d), 4) * 128, 128)
                for x in range(4):
                    panel_ref[x, pl.ds(at, 128), 256 * c : 256 * (c + 1)] = near[d][x]
                    panel_ref[x, pl.ds(at, 128), 256 * (1 - c) : 256 * (2 - c)] = far[d][x]

    inverse_into(panel_ref.at[z], inverse_ref)
    first_ref[...] = dot_nt(rows_ref[...], inverse_ref[...])


def in_vmem():
    return pl.BlockSpec(memory_space=pltpu.VMEM)


def in_smem():
    return pl.BlockSpec(memory_space=pltpu.SMEM)


def prepare(place, rows, near, far):
    return pl.pallas_call(
        prepare_body,
        in_specs=[in_smem()] + [in_vmem()] * 9,
        out_specs=[in_vmem()] * 3,
        out_shape=[
            jax.ShapeDtypeStruct((4, 512, 512), jnp.float32),
            jax.ShapeDtypeStruct((512, 512), jnp.float32),
            jax.ShapeDtypeStruct((192, 512), jnp.float32),
        ],
        name="prepare",
    )(place, rows, *near, *far)


def step_body(k, place_ref, rows_ref, panel_ref, inverse_ref, own_ref, p1_ref, p2_ref, p3_ref, *outs):
    z = place_ref[2]
    mine_ref = outs[0]
    for d, ref in enumerate((own_ref, p1_ref, p2_ref, p3_ref)):

        @pl.when(z == (k + d) % 4)
        def _():
            mine_ref[...] = ref[...]

    if k < 3:
        rest = rows_ref[...] - dot_nt(mine_ref[...], panel_ref[0])
        outs[1][...] = rest
        outs[2][...] = dot_nt(rest, inverse_ref[...])


def step(k, place, rows, panel, inverse, own, arrived):
    piece = jax.ShapeDtypeStruct((192, 512), jnp.float32)
    count = 3 if k < 3 else 1
    whole = pl.BlockSpec((192, 512), lambda i: (0, 0))
    return pl.pallas_call(
        functools.partial(step_body, k),
        grid=(1,),
        in_specs=[in_smem(), whole, pl.BlockSpec((1, 512, 512), lambda i: (k, 0, 0)), pl.BlockSpec((512, 512), lambda i: (0, 0))]
        + [whole] * 4,
        out_specs=[whole] * count,
        out_shape=[piece] * count,
        name="step",
    )(place, rows, panel, inverse, own, *arrived)


def pack_body(place_ref, own_ref, m1_ref, m2_ref, m3_ref, *rest):
    solved_ref, high_ref, low_ref = rest[-3:]
    core, y = place_ref[0], place_ref[1]
    for d, ref in enumerate((own_ref, m1_ref, m2_ref, m3_ref)):
        at = pl.multiple_of(lax.rem(y + (4 - d), 4) * 192, 192)
        value = ref[...]
        solved_ref[pl.ds(at, 192), :] = value
        left, right = value[:, :256], value[:, 256:]
        value = jnp.concatenate([jnp.where(core == 0, left, right), jnp.where(core == 0, right, left)], axis=1)
        high = value.astype(jnp.bfloat16)
        high_ref[pl.ds(at, 192), :] = high
        low_ref[pl.ds(at, 192), :] = (value - high.astype(jnp.float32)).astype(jnp.bfloat16)


def pack(k, place, pieces, into):
    piece = pl.BlockSpec((192, 512), lambda i: (0, 0))
    column = pl.BlockSpec((768, 512), lambda i: (0, k))
    operands = [place, *pieces]
    specs = [in_smem()] + [piece] * 4
    aliases = {}
    if into is not None:
        operands += into
        specs += [pl.BlockSpec(memory_space=pl.ANY)] * 3
        aliases = {5: 0, 6: 1, 7: 2}
    return pl.pallas_call(
        pack_body,
        grid=(1,),
        in_specs=specs,
        out_specs=[column] * 3,
        out_shape=[jax.ShapeDtypeStruct((768, 2048), t) for t in (jnp.float32, jnp.bfloat16, jnp.bfloat16)],
        input_output_aliases=aliases,
        name="pack",
    )(*operands)


def update_body(first, block_ref, a_ref, xh_ref, xl_ref, own_ref, other_ref, *rest):
    out_ref, high_ref, low_ref = rest[-3:]
    block_id = block_ref[3] + (first + pl.program_id(0)) * 16
    for half, ref in ((0, own_ref), (1, other_ref)):
        for x in range(4):
            at = x * 512 + half * 256
            part = jnp.where(x < block_id, ref[x, 0], 0.0)
            high = part.astype(jnp.bfloat16)
            high_ref[:, at : at + 256] = high
            low_ref[:, at : at + 256] = (part - high.astype(jnp.float32)).astype(jnp.bfloat16)
    dims = (((1,), (1,)), ((), ()))
    high, low = high_ref[...], low_ref[...]
    total = lax.dot_general(xh_ref[...], high, dims, preferred_element_type=jnp.float32)
    total += lax.dot_general(xh_ref[...], low, dims, preferred_element_type=jnp.float32)
    total += lax.dot_general(xl_ref[...], high, dims, preferred_element_type=jnp.float32)
    out_ref[0] = a_ref[0] - total


def update(first, count, block, a, xh, xl, own, other, into=None):
    rows, width = a.shape[1], a.shape[2]
    tb = 256
    big = pl.BlockSpec((1, rows, tb), lambda l, t: (first + l, 0, t))
    tiles = pl.BlockSpec((4, 1, tb, 256), lambda l, t: (0, l, t, 0))
    whole = pl.BlockSpec(xh.shape, lambda l, t: (0, 0))
    operands = [block, a, xh, xl, own, other]
    specs = [pl.BlockSpec(memory_space=pltpu.SMEM), big, whole, whole, tiles, tiles]
    aliases = {}
    if into is not None:
        operands.append(into)
        specs.append(pl.BlockSpec(memory_space=pl.ANY))
        aliases = {6: 0}
    return pl.pallas_call(
        functools.partial(update_body, first),
        grid=(count, width // tb),
        in_specs=specs,
        out_specs=big,
        out_shape=jax.ShapeDtypeStruct(a.shape, jnp.float32),
        scratch_shapes=[pltpu.VMEM((tb, 2048), jnp.bfloat16), pltpu.VMEM((tb, 2048), jnp.bfloat16)],
        input_output_aliases=aliases,
        compiler_params=pltpu.CompilerParams(vmem_limit_bytes=48 * 1024 * 1024),
        name="update",
    )(*operands)


def ring(shift):
    return [(i, (i + shift) % 4) for i in range(4)]


def over_z(value, k):
    return [lax.ppermute(value, "z", [(k, (k + d) % 4)]) for d in (1, 2, 3)]


def over_y(value):
    return [value] + [lax.ppermute(value, "y", ring(d)) for d in (1, 2, 3)]


def placed(matrix, factor):
    core, y, z = lax.axis_index("core"), lax.axis_index("y"), lax.axis_index("z")
    place = jnp.stack([core, y, z, y * 4 + z]).astype(jnp.int32)
    a = matrix.transpose(1, 0, 2)

    def sent(j):
        top = a[0, 192 * j : 192 * (j + 1)]
        return jnp.concatenate([top[:, :256], top[:, 256:], factor[0, 128 * j : 128 * (j + 1)]], axis=0)

    start = sent(0)
    for j in range(1, 4):
        start = jnp.where(y == j, lax.ppermute(sent(j), "y", [(0, j)]), start)
    rows = jnp.concatenate([start[:192], start[192:384]], axis=1)
    tile = lax.all_gather(start[384:], "x")
    near = over_y(tile)
    far = [lax.ppermute(t, "core", SWAP) for t in near]
    panel, inverse, candidate = prepare(place, rows, near, far)

    bulk = []
    for first in (0, 3):
        piece = lax.all_gather(factor[first : first + 3], "x")
        bulk.append((piece, lax.ppermute(piece, "core", SWAP)))

    packed = None
    for k in range(4):
        moved = over_z(candidate, k)
        done = step(k, place, rows, panel, inverse, candidate, moved)
        if k < 3:
            mine, rows, candidate = done
        else:
            mine = done[0]
        pieces = over_y(mine)
        packed = pack(k, place, pieces, packed)
    solved, high, low = packed

    out = update(0, 3, place, a, high, low, *bulk[0])
    out = update(3, 3, place, a, high, low, *bulk[1], out)
    return out.transpose(1, 0, 2), solved


def solution(mesh):
    finer = Mesh(mesh.devices.reshape(4, 2, 4, 4), (*ROW, *COL))
    return jax.shard_map(
        placed,
        mesh=finer,
        in_specs=(P(ROW, None, COL), P(None, COL, ROW)),
        out_specs=(P(ROW, None, COL), P(ROW, None)),
        check_vma=False,
    )
```

```python
import functools

import jax
import jax.numpy as jnp
from jax import lax
from jax.experimental import pallas as pl
from jax.experimental.pallas import tpu as pltpu
from jax.sharding import Mesh
from jax.sharding import PartitionSpec as P


ROW = ("x", "core")
COL = ("y", "z")
SWAP = [(0, 1), (1, 0)]
HIGHEST = lax.Precision.HIGHEST


def full_dot(a, b):
    return jnp.dot(a, b, precision=HIGHEST, preferred_element_type=jnp.float32)


def dot_nt(a, b):
    return lax.dot_general(
        a, b, (((1,), (1,)), ((), ())), precision=HIGHEST, preferred_element_type=jnp.float32
    )


def inverse_into(tile_ref, out_ref):
    size, wide, small = 512, 128, 16
    parts = size // wide
    diag = jnp.concatenate(
        [tile_ref[wide * p : wide * (p + 1), wide * p : wide * (p + 1)] for p in range(parts)], axis=0
    )
    row = lax.broadcasted_iota(jnp.int32, (size, wide), 0)
    lane = lax.broadcasted_iota(jnp.int32, (size, wide), 1)
    local_row = row % wide
    lower = jnp.where(lane <= local_row, diag, 0.0)
    own = jnp.sum(jnp.where(lane == local_row, lower, 0.0), axis=1, keepdims=True)
    unit = lower / own
    inverse = jnp.where(lane == local_row, 1.0, 0.0)
    block_start = (local_row // small) * small
    inverse = inverse.reshape(size // small, small, wide)
    for i in range(small - 1):
        picked = jnp.where((lane == block_start + i) & (local_row > lane), unit, 0.0)
        weight = jnp.sum(picked, axis=1, keepdims=True).reshape(size // small, small, 1)
        inverse = inverse - weight * inverse[:, i : i + 1, :]
    inverse = inverse.reshape(size, wide)
    r1 = lax.broadcasted_iota(jnp.int32, (wide, wide), 0)
    c1 = lax.broadcasted_iota(jnp.int32, (wide, wide), 1)
    invs = [inverse[wide * p : wide * (p + 1)] for p in range(parts)]
    step = small
    while step < wide:
        keep = (r1 // (2 * step) == c1 // (2 * step)) & (r1 // step > c1 // step)
        offs = [jnp.where(keep, unit[wide * p : wide * (p + 1)], 0.0) for p in range(parts)]
        mids = [full_dot(offs[p], invs[p]) for p in range(parts)]
        invs = [invs[p] - full_dot(invs[p], mids[p]) for p in range(parts)]
        step *= 2
    out_ref[...] = jnp.zeros((size, size), jnp.float32)
    for p in range(parts):
        scale = jnp.broadcast_to(1.0 / own[wide * p : wide * (p + 1)], (wide, wide))
        as_row = jnp.sum(jnp.where(r1 == c1, scale, 0.0), axis=0, keepdims=True)
        out_ref[wide * p : wide * (p + 1), wide * p : wide * (p + 1)] = invs[p] * as_row
    step = wide
    while step < size:
        for s in range(0, size, 2 * step):
            top = out_ref[s : s + step, s : s + step]
            bottom = out_ref[s + step : s + 2 * step, s + step : s + 2 * step]
            between = tile_ref[s + step : s + 2 * step, s : s + step]
            out_ref[s + step : s + 2 * step, s : s + step] = -full_dot(bottom, full_dot(between, top))
        step *= 2


def by_core(place_ref, rows, put):
    core, y = place_ref[0], place_ref[1]
    for c in range(2):

        @pl.when(core == c)
        def _():
            for d in range(4):
                at = pl.multiple_of(lax.rem(y + (4 - d), 4) * rows, rows)
                put(d, pl.ds(at, rows), 256 * c, 256 * (1 - c))


def invert_body(place_ref, rows_ref, near_ref, far_ref, inverse_ref, first_ref, tile_ref):
    def put(d, at, here, there):
        tile_ref[at, here : here + 256] = near_ref[d]
        tile_ref[at, there : there + 256] = far_ref[d]

    by_core(place_ref, 128, put)
    inverse_into(tile_ref, inverse_ref)
    first_ref[...] = dot_nt(rows_ref[...], inverse_ref[...])


def gain_body(place_ref, inverse_ref, near_ref, far_ref, gain_ref, tile_ref):
    def put(d, at, here, there):
        for x in range(3):
            tile_ref[at, 512 * x + here : 512 * x + here + 256] = near_ref[d, x]
            tile_ref[at, 512 * x + there : 512 * x + there + 256] = far_ref[d, x]

    by_core(place_ref, 128, put)
    for x in range(3):
        gain_ref[x] = full_dot(inverse_ref[...], tile_ref[:, 512 * x : 512 * (x + 1)]).T


def in_vmem():
    return pl.BlockSpec(memory_space=pltpu.VMEM)


def in_smem():
    return pl.BlockSpec(memory_space=pltpu.SMEM)


def f32(*shape):
    return jax.ShapeDtypeStruct(shape, jnp.float32)


def invert(place, rows, near, far):
    return pl.pallas_call(
        invert_body,
        in_specs=[in_smem()] + [in_vmem()] * 3,
        out_specs=[in_vmem()] * 2,
        out_shape=[f32(512, 512), f32(192, 512)],
        scratch_shapes=[pltpu.VMEM((512, 512), jnp.float32)],
        name="invert",
    )(place, rows, near, far)


def gain(place, inverse, near, far):
    return pl.pallas_call(
        gain_body,
        in_specs=[in_smem()] + [in_vmem()] * 3,
        out_specs=in_vmem(),
        out_shape=f32(3, 512, 512),
        scratch_shapes=[pltpu.VMEM((512, 1536), jnp.float32)],
        name="gain",
    )(place, inverse, near, far)


def step_body(k, place_ref, left_ref, gain_ref, next_ref, out_ref):
    z = place_ref[2]

    @pl.when(z == k + 1)
    def _():
        out_ref[...] = left_ref[...] - full_dot(next_ref[...], gain_ref[0])

    @pl.when(z != k + 1)
    def _():
        out_ref[...] = left_ref[...]


def late_body(k, place_ref, own_ref, p1_ref, p2_ref, p3_ref, *rest):
    z = place_ref[2]
    mine_ref = rest[2] if len(rest) > 1 else rest[0]
    for d, ref in enumerate((own_ref, p1_ref, p2_ref, p3_ref)):

        @pl.when(z == (k + d) % 4)
        def _():
            mine_ref[...] = ref[...]

    if len(rest) > 1:
        left_ref, gain_ref, _, out_ref = rest

        @pl.when(z > k + 1)
        def _():
            out_ref[...] = left_ref[...] - full_dot(mine_ref[...], gain_ref[0])

        @pl.when(z <= k + 1)
        def _():
            out_ref[...] = left_ref[...]


def piece_spec():
    return pl.BlockSpec((192, 512), lambda i: (0, 0))


def gain_spec(k):
    return pl.BlockSpec((1, 512, 512), lambda i: (k, 0, 0))


def step(k, place, left, gains, arrived):
    return pl.pallas_call(
        functools.partial(step_body, k),
        grid=(1,),
        in_specs=[in_smem(), piece_spec(), gain_spec(k), piece_spec()],
        out_specs=piece_spec(),
        out_shape=f32(192, 512),
        name="step",
    )(place, left, gains, arrived)


def late(k, place, own, arrived, left=None, gains=None):
    more = left is not None
    return pl.pallas_call(
        functools.partial(late_body, k),
        grid=(1,),
        in_specs=[in_smem()] + [piece_spec()] * 4 + ([piece_spec(), gain_spec(k)] if more else []),
        out_specs=[piece_spec()] * (2 if more else 1),
        out_shape=[f32(192, 512)] * (2 if more else 1),
        name="late",
    )(place, own, *arrived, *((left, gains) if more else ()))


def pack_body(place_ref, own_ref, m1_ref, m2_ref, m3_ref, *rest):
    solved_ref, high_ref, low_ref = rest[-3:]
    core, y = place_ref[0], place_ref[1]
    for d, ref in enumerate((own_ref, m1_ref, m2_ref, m3_ref)):
        at = pl.multiple_of(lax.rem(y + (4 - d), 4) * 192, 192)
        value = ref[...]
        solved_ref[pl.ds(at, 192), :] = value
        left, right = value[:, :256], value[:, 256:]
        for half in range(2):
            part = jnp.where(core == half, left, right)
            high = part.astype(jnp.bfloat16)
            high_ref[half, pl.ds(at, 192), :] = high
            low_ref[half, pl.ds(at, 192), :] = (part - high.astype(jnp.float32)).astype(jnp.bfloat16)


def pack(k, place, pieces, into):
    operands = [place, *pieces]
    specs = [in_smem()] + [piece_spec()] * 4
    aliases = {}
    if into is not None:
        operands.append(into)
        specs.append(pl.BlockSpec(memory_space=pl.ANY))
        aliases = {5: 0}
    part = jax.ShapeDtypeStruct((2, 768, 256), jnp.bfloat16)
    part_spec = pl.BlockSpec((2, 768, 256), lambda i: (0, 0, 0))
    return pl.pallas_call(
        pack_body,
        grid=(1,),
        in_specs=specs,
        out_specs=[pl.BlockSpec((768, 512), lambda i: (0, k)), part_spec, part_spec],
        out_shape=[f32(768, 2048), part, part],
        input_output_aliases=aliases,
        name="pack",
    )(*operands)


def update_body(halves, first, count, block_ref, into_ref, *refs):
    xs, tiles = refs[: 2 * count], refs[2 * count : 2 * count + len(halves)]
    out_ref, high_ref, low_ref, xh_ref, xl_ref = refs[-5:]

    @pl.when(pl.program_id(0) == 0)
    def _():
        for p in range(count):
            for h in range(len(halves)):
                at = (p * len(halves) + h) * 256
                xh_ref[:, at : at + 256] = xs[2 * p][h]
                xl_ref[:, at : at + 256] = xs[2 * p + 1][h]

    block_id = block_ref[3] + pl.program_id(0) * 16
    for p in range(count):
        for h in range(len(halves)):
            at = (p * len(halves) + h) * 256
            part = jnp.where(first + p < block_id, tiles[h][p, 0], 0.0)
            high = part.astype(jnp.bfloat16)
            high_ref[:, at : at + 256] = high
            low_ref[:, at : at + 256] = (part - high.astype(jnp.float32)).astype(jnp.bfloat16)
    dims = (((1,), (1,)), ((), ()))
    high, low = high_ref[...], low_ref[...]
    total = lax.dot_general(xh_ref[...], high, dims, preferred_element_type=jnp.float32)
    total += lax.dot_general(xh_ref[...], low, dims, preferred_element_type=jnp.float32)
    total += lax.dot_general(xl_ref[...], high, dims, preferred_element_type=jnp.float32)
    out_ref[0] = into_ref[0] - total


def update(halves, first, place, into, xs, tiles, alias):
    count = len(xs)
    blocks, rows, width = into.shape
    big = pl.BlockSpec((1, rows, width), lambda l: (l, 0, 0))
    tile_spec = pl.BlockSpec((count, 1, width, 256), lambda l: (first // count, l, 0, 0))
    x_spec = pl.BlockSpec((len(halves), rows, 256), lambda l: (halves[0], 0, 0))
    depth = 256 * count * len(halves)
    return pl.pallas_call(
        functools.partial(update_body, halves, first, count),
        grid=(blocks,),
        in_specs=[in_smem(), big] + [x_spec] * (2 * count) + [tile_spec] * len(halves),
        out_specs=big,
        out_shape=f32(*into.shape),
        scratch_shapes=[pltpu.VMEM((width, depth), jnp.bfloat16)] * 2 + [pltpu.VMEM((rows, depth), jnp.bfloat16)] * 2,
        input_output_aliases={1: 0} if alias else {},
        compiler_params=pltpu.CompilerParams(vmem_limit_bytes=48 * 1024 * 1024),
        name="update",
    )(place, into, *[part for x in xs for part in x], *tiles)


def ring(shift):
    return [(i, (i + shift) % 4) for i in range(4)]


def over_z(value, k):
    return [lax.ppermute(value, "z", [(k, (k + d) % 4)]) for d in (1, 2, 3)]


def over_y(value):
    return [value] + [lax.ppermute(value, "y", ring(d)) for d in (1, 2, 3)]


def spread(piece, y):
    out = piece(0)
    moved = [lax.ppermute(piece(j), "y", [(0, j)]) for j in range(1, 4)]
    for j in range(1, 4):
        out = jnp.where(y == j, moved[j - 1], out)
    return out


def placed(matrix, factor):
    core, y, z = lax.axis_index("core"), lax.axis_index("y"), lax.axis_index("z")
    place = jnp.stack([core, y, z, y * 4 + z]).astype(jnp.int32)
    a = matrix.transpose(1, 0, 2)

    near = lax.all_gather(factor, "x")
    far = lax.ppermute(near, "core", SWAP)

    tile = spread(lambda j: factor[0, 128 * j : 128 * (j + 1)], y)
    rows = spread(lambda j: a[0, 192 * j : 192 * (j + 1)], y)
    tile = lax.all_gather(tile, "x")
    diag = jnp.stack(over_y(lax.dynamic_index_in_dim(tile, z, 0, keepdims=False)))
    diag_far = lax.ppermute(diag, "core", SWAP)
    inverse, left = invert(place, rows, diag, diag_far)
    pieces = over_y(tile[:3])
    off = jnp.stack(pieces)
    off_far = lax.ppermute(off, "core", SWAP)
    gains = gain(place, inverse, off, off_far)

    solved, parts, before = None, [], None

    def finish(k, mine, solved):
        pieces = over_y(mine)
        solved, high, low = pack(k, place, pieces, solved)
        parts.append((high, low))
        return solved

    for k in range(4):
        sent, moved = left, over_z(left, k)
        if k > 0:
            if k < 3:
                mine, left = late(k - 1, place, *before, left, gains)
            else:
                (mine,) = late(k - 1, place, *before)
            solved = finish(k - 1, mine, solved)
        if k < 3:
            left = step(k, place, left, gains, moved[0])
        before = (sent, moved)
    (mine,) = late(3, place, *before)
    solved = finish(3, mine, solved)

    out = update((0,), 0, place, a, parts[:3], [near], False)
    out = update((1,), 0, place, out, parts[:3], [far], True)
    out = update((0, 1), 3, place, out, parts[3:], [near, far], True)
    return out.transpose(1, 0, 2), solved


def solution(mesh):
    finer = Mesh(mesh.devices.reshape(4, 2, 4, 4), (*ROW, *COL))
    return jax.shard_map(
        placed,
        mesh=finer,
        in_specs=(P(ROW, None, COL), P(None, COL, ROW)),
        out_specs=(P(ROW, None, COL), P(ROW, None)),
        check_vma=False,
    )
```

```python
import functools

import jax
import jax.numpy as jnp
from jax import lax
from jax.experimental import pallas as pl
from jax.experimental.pallas import tpu as pltpu
from jax.sharding import Mesh
from jax.sharding import PartitionSpec as P


ROW = ("x", "core")
COL = ("y", "z")
SWAP = [(0, 1), (1, 0)]
HIGHEST = lax.Precision.HIGHEST


def full_dot(a, b):
    return jnp.dot(a, b, precision=HIGHEST, preferred_element_type=jnp.float32)


def dot_nt(a, b):
    return lax.dot_general(
        a, b, (((1,), (1,)), ((), ())), precision=HIGHEST, preferred_element_type=jnp.float32
    )


def inverse_into(tile_ref, out_ref):
    size, wide, small = 512, 128, 16
    parts = size // wide
    diag = jnp.concatenate(
        [tile_ref[wide * p : wide * (p + 1), wide * p : wide * (p + 1)] for p in range(parts)], axis=0
    )
    row = lax.broadcasted_iota(jnp.int32, (size, wide), 0)
    lane = lax.broadcasted_iota(jnp.int32, (size, wide), 1)
    local_row = row % wide
    lower = jnp.where(lane <= local_row, diag, 0.0)
    own = jnp.sum(jnp.where(lane == local_row, lower, 0.0), axis=1, keepdims=True)
    unit = lower / own
    inverse = jnp.where(lane == local_row, 1.0, 0.0)
    block_start = (local_row // small) * small
    inverse = inverse.reshape(size // small, small, wide)
    for i in range(small - 1):
        picked = jnp.where((lane == block_start + i) & (local_row > lane), unit, 0.0)
        weight = jnp.sum(picked, axis=1, keepdims=True).reshape(size // small, small, 1)
        inverse = inverse - weight * inverse[:, i : i + 1, :]
    inverse = inverse.reshape(size, wide)
    r1 = lax.broadcasted_iota(jnp.int32, (wide, wide), 0)
    c1 = lax.broadcasted_iota(jnp.int32, (wide, wide), 1)
    invs = [inverse[wide * p : wide * (p + 1)] for p in range(parts)]
    step = small
    while step < wide:
        keep = (r1 // (2 * step) == c1 // (2 * step)) & (r1 // step > c1 // step)
        offs = [jnp.where(keep, unit[wide * p : wide * (p + 1)], 0.0) for p in range(parts)]
        mids = [full_dot(offs[p], invs[p]) for p in range(parts)]
        invs = [invs[p] - full_dot(invs[p], mids[p]) for p in range(parts)]
        step *= 2
    out_ref[...] = jnp.zeros((size, size), jnp.float32)
    for p in range(parts):
        scale = jnp.broadcast_to(1.0 / own[wide * p : wide * (p + 1)], (wide, wide))
        as_row = jnp.sum(jnp.where(r1 == c1, scale, 0.0), axis=0, keepdims=True)
        out_ref[wide * p : wide * (p + 1), wide * p : wide * (p + 1)] = invs[p] * as_row
    step = wide
    while step < size:
        for s in range(0, size, 2 * step):
            top = out_ref[s : s + step, s : s + step]
            bottom = out_ref[s + step : s + 2 * step, s + step : s + 2 * step]
            between = tile_ref[s + step : s + 2 * step, s : s + step]
            out_ref[s + step : s + 2 * step, s : s + step] = -full_dot(bottom, full_dot(between, top))
        step *= 2


def by_core(place_ref, rows, put):
    core, y = place_ref[0], place_ref[1]
    for c in range(2):

        @pl.when(core == c)
        def _():
            for d in range(4):
                at = pl.multiple_of(lax.rem(y + (4 - d), 4) * rows, rows)
                put(d, pl.ds(at, rows), 256 * c, 256 * (1 - c))


def invert_body(place_ref, rows_ref, near_ref, far_ref, inverse_ref, first_ref, tile_ref):
    def put(d, at, here, there):
        tile_ref[at, here : here + 256] = near_ref[d]
        tile_ref[at, there : there + 256] = far_ref[d]

    by_core(place_ref, 128, put)
    inverse_into(tile_ref, inverse_ref)
    inverse_ref[...] = inverse_ref[...].T
    first_ref[...] = full_dot(rows_ref[...], inverse_ref[...])


def tile_into(place_ref, near_ref, far_ref, tile_ref):
    def put(d, at, here, there):
        tile_ref[at, here : here + 256] = near_ref[d, 0]
        tile_ref[at, there : there + 256] = far_ref[d, 0]

    by_core(place_ref, 128, put)


def in_vmem():
    return pl.BlockSpec(memory_space=pltpu.VMEM)


def in_smem():
    return pl.BlockSpec(memory_space=pltpu.SMEM)


def f32(*shape):
    return jax.ShapeDtypeStruct(shape, jnp.float32)


def invert(place, rows, near, far):
    return pl.pallas_call(
        invert_body,
        in_specs=[in_smem()] + [in_vmem()] * 3,
        out_specs=[in_vmem()] * 2,
        out_shape=[f32(512, 512), f32(192, 512)],
        scratch_shapes=[pltpu.VMEM((512, 512), jnp.float32)],
        name="invert",
    )(place, rows, near, far)


def step_body(k, place_ref, left_ref, near_ref, far_ref, inverse_ref, next_ref, out_ref, tile_ref):
    z = place_ref[2]

    @pl.when(z == k + 1)
    def _():
        tile_into(place_ref, near_ref, far_ref, tile_ref)
        rest = left_ref[...] - dot_nt(next_ref[...], tile_ref[...])
        out_ref[...] = full_dot(rest, inverse_ref[...])

    @pl.when(z != k + 1)
    def _():
        out_ref[...] = jnp.zeros((192, 512), jnp.float32)


def late_body(k, place_ref, own_ref, p1_ref, p2_ref, p3_ref, *rest):
    z = place_ref[2]
    mine_ref = rest[3] if len(rest) > 1 else rest[0]
    for d, ref in enumerate((own_ref, p1_ref, p2_ref, p3_ref)):

        @pl.when(z == (k + d) % 4)
        def _():
            mine_ref[...] = ref[...]

    if len(rest) > 1:
        left_ref, near_ref, far_ref, _, out_ref, tile_ref = rest

        @pl.when(z > k + 1)
        def _():
            tile_into(place_ref, near_ref, far_ref, tile_ref)
            out_ref[...] = left_ref[...] - dot_nt(mine_ref[...], tile_ref[...])

        @pl.when(z <= k + 1)
        def _():
            out_ref[...] = left_ref[...]


def piece_spec():
    return pl.BlockSpec((192, 512), lambda i: (0, 0))


def side_specs(k):
    return [pl.BlockSpec((4, 1, 128, 256), lambda i: (0, k, 0, 0))] * 2


def tile_scratch():
    return [pltpu.VMEM((512, 512), jnp.float32)]


def step(k, place, left, sides, inverse, arrived):
    return pl.pallas_call(
        functools.partial(step_body, k),
        grid=(1,),
        in_specs=[in_smem(), piece_spec(), *side_specs(k), pl.BlockSpec((512, 512), lambda i: (0, 0)), piece_spec()],
        out_specs=piece_spec(),
        out_shape=f32(192, 512),
        scratch_shapes=tile_scratch(),
        name="step",
    )(place, left, *sides, inverse, arrived)


def late(k, place, own, arrived, left=None, sides=None):
    more = left is not None
    return pl.pallas_call(
        functools.partial(late_body, k),
        grid=(1,),
        in_specs=[in_smem()] + [piece_spec()] * 4 + ([piece_spec(), *side_specs(k)] if more else []),
        out_specs=[piece_spec()] * (2 if more else 1),
        out_shape=[f32(192, 512)] * (2 if more else 1),
        scratch_shapes=tile_scratch() if more else [],
        name="late",
    )(place, own, *arrived, *((left, *sides) if more else ()))


def pack_body(place_ref, own_ref, m1_ref, m2_ref, m3_ref, *rest):
    solved_ref, high_ref, low_ref = rest[-3:]
    core, y = place_ref[0], place_ref[1]
    for d, ref in enumerate((own_ref, m1_ref, m2_ref, m3_ref)):
        at = pl.multiple_of(lax.rem(y + (4 - d), 4) * 192, 192)
        value = ref[...]
        solved_ref[pl.ds(at, 192), :] = value
        left, right = value[:, :256], value[:, 256:]
        for half in range(2):
            part = jnp.where(core == half, left, right)
            high = part.astype(jnp.bfloat16)
            high_ref[half, pl.ds(at, 192), :] = high
            low_ref[half, pl.ds(at, 192), :] = (part - high.astype(jnp.float32)).astype(jnp.bfloat16)


def pack(k, place, pieces, into):
    operands = [place, *pieces]
    specs = [in_smem()] + [piece_spec()] * 4
    aliases = {}
    if into is not None:
        operands.append(into)
        specs.append(pl.BlockSpec(memory_space=pl.ANY))
        aliases = {5: 0}
    part = jax.ShapeDtypeStruct((2, 768, 256), jnp.bfloat16)
    part_spec = pl.BlockSpec((2, 768, 256), lambda i: (0, 0, 0))
    return pl.pallas_call(
        pack_body,
        grid=(1,),
        in_specs=specs,
        out_specs=[pl.BlockSpec((768, 512), lambda i: (0, k)), part_spec, part_spec],
        out_shape=[f32(768, 2048), part, part],
        input_output_aliases=aliases,
        name="pack",
    )(*operands)


def update_body(spans, place_ref, into_ref, *refs):
    items = [(p, h, s, p - start) for s, (h, start, count) in enumerate(spans) for p in range(start, start + count)]
    xs, tiles = refs[: 2 * len(items)], refs[2 * len(items) : 2 * len(items) + len(spans)]
    out_ref, tile_ref, x_ref = refs[-3:]
    depth = 256 * len(items)

    @pl.when(pl.program_id(0) == 0)
    def _():
        for i in range(len(items)):
            high, low = xs[2 * i][0], xs[2 * i + 1][0]
            x_ref[:, 256 * i : 256 * (i + 1)] = high
            x_ref[:, depth + 256 * i : depth + 256 * (i + 1)] = high
            x_ref[:, 2 * depth + 256 * i : 2 * depth + 256 * (i + 1)] = low

    block_id = place_ref[3] + pl.program_id(0) * 16
    for i, (panel, _, span, at) in enumerate(items):
        part = jnp.where(panel < block_id, tiles[span][at, 0], 0.0)
        high = part.astype(jnp.bfloat16)
        tile_ref[:, 256 * i : 256 * (i + 1)] = high
        tile_ref[:, depth + 256 * i : depth + 256 * (i + 1)] = (part - high.astype(jnp.float32)).astype(jnp.bfloat16)
        tile_ref[:, 2 * depth + 256 * i : 2 * depth + 256 * (i + 1)] = high
    out_ref[0] = into_ref[0] - lax.dot_general(
        x_ref[...], tile_ref[...], (((1,), (1,)), ((), ())), preferred_element_type=jnp.float32
    )


def update(spans, place, into, parts, bulk, alias):
    blocks, rows, width = into.shape
    big = pl.BlockSpec((1, rows, width), lambda l: (l, 0, 0))
    operands, specs = [place, into], [in_smem(), big]
    for h, start, count in spans:
        for p in range(start, start + count):
            operands += parts[p]
            specs += [pl.BlockSpec((1, rows, 256), lambda l, h=h: (h, 0, 0))] * 2
    for h, start, count in spans:
        operands.append(bulk[h])
        specs.append(pl.BlockSpec((count, 1, width, 256), lambda l, at=start // count: (at, l, 0, 0)))
    depth = 3 * 256 * sum(count for _, _, count in spans)
    return pl.pallas_call(
        functools.partial(update_body, spans),
        grid=(blocks,),
        in_specs=specs,
        out_specs=big,
        out_shape=f32(*into.shape),
        scratch_shapes=[pltpu.VMEM((width, depth), jnp.bfloat16), pltpu.VMEM((rows, depth), jnp.bfloat16)],
        input_output_aliases={1: 0} if alias else {},
        compiler_params=pltpu.CompilerParams(vmem_limit_bytes=52 * 1024 * 1024),
        name="update",
    )(*operands)


def ring(shift):
    return [(i, (i + shift) % 4) for i in range(4)]


def over_z(value, k):
    up = lax.ppermute(value, "z", [(k, (k + 1) % 4)])
    down = lax.ppermute(value, "z", [(k, (k + 3) % 4)])
    on = lax.ppermute(down, "z", [((k + 3) % 4, (k + 2) % 4)])
    return [up, on, down]


def over_y(value):
    return [value] + [lax.ppermute(value, "y", ring(d)) for d in (1, 2, 3)]


def spread(piece, y):
    out = piece(0)
    moved = [lax.ppermute(piece(j), "y", [(0, j)]) for j in range(1, 4)]
    for j in range(1, 4):
        out = jnp.where(y == j, moved[j - 1], out)
    return out


def placed(matrix, factor):
    core, y, z = lax.axis_index("core"), lax.axis_index("y"), lax.axis_index("z")
    place = jnp.stack([core, y, z, y * 4 + z]).astype(jnp.int32)
    a = matrix.transpose(1, 0, 2)

    near = lax.all_gather(factor, "x")
    far = lax.ppermute(near, "core", SWAP)

    tile = spread(lambda j: factor[0, 128 * j : 128 * (j + 1)], y)
    rows = spread(lambda j: a[0, 192 * j : 192 * (j + 1)], y)
    tile = lax.all_gather(tile, "x")
    diag = jnp.stack(over_y(lax.dynamic_index_in_dim(tile, z, 0, keepdims=False)))
    diag_far = lax.ppermute(diag, "core", SWAP)
    inverse, ready = invert(place, rows, diag, diag_far)
    pieces = over_y(tile[:3])
    off = jnp.stack(pieces)
    off_far = lax.ppermute(off, "core", SWAP)
    sides, left = (off, off_far), rows

    solved, parts, before = None, [], None

    def finish(k, mine, solved):
        pieces = over_y(mine)
        solved, high, low = pack(k, place, pieces, solved)
        parts.append((high, low))
        return solved

    for k in range(4):
        sent, moved = ready, over_z(ready, k)
        if k > 0:
            if k < 3:
                mine, left = late(k - 1, place, *before, left, sides)
            else:
                (mine,) = late(k - 1, place, *before)
            solved = finish(k - 1, mine, solved)
        if k < 3:
            ready = step(k, place, left, sides, inverse, moved[0])
        before = (sent, moved)
    (mine,) = late(3, place, *before)
    solved = finish(3, mine, solved)

    out = update(((0, 0, 2),), place, a, parts, (near, far), False)
    out = update(((0, 2, 2), (1, 0, 4)), place, out, parts, (near, far), True)
    return out.transpose(1, 0, 2), solved


def solution(mesh):
    finer = Mesh(mesh.devices.reshape(4, 2, 4, 4), (*ROW, *COL))
    return jax.shard_map(
        placed,
        mesh=finer,
        in_specs=(P(ROW, None, COL), P(None, COL, ROW)),
        out_specs=(P(ROW, None, COL), P(ROW, None)),
        check_vma=False,
    )
```
